32 devices in a mesh: wall: 8 (over z, x), spec: 4 (over y, core).
Axes of the slice: x: 2, y: 2, z: 4, core: 2. Of those that a mesh axis runs over, the one named last changes fastest.
Arguments:
- signal: bfloat16 [4, 2, 256, 32, 10240], P(None, None, 'wall', None, 'spec'), may hold values from -6 to 6
- kx_index: int32 [128], replicated, may hold values from 0 to 5119
- kz_index: int32 [128], replicated, may hold values from 0 to 3
Outputs:
- phi: float32 [2, 128, 256, 256], P(None, 'spec', 'wall')
The draws below stay inside these ranges and needn't reach their ends.
Inputs may be any that keep to these rules, and one draw needn't show every extreme that they name: `kx_index`: pairs may repeat.
All inputs are finite; a program needn't handle non-finite values.
Results may differ from the reference program's by a relative error of at most 0.0042.
Values sent between devices are 32-bit elements; how exact they have to be, the bound alone decides.
A program may use at most 128 MiB of HBM per device.

```python
import math
import jax
import jax.numpy as jnp
from jax import lax

NXW = 10240
K = 128
KZ = 4
SNAP = 32
NY = 256


def plant(result, rng, smallest, top_value):
    extent = result.shape
    index_at = [jax.random.randint(jax.random.fold_in(rng, axis), (), 0, extent[axis]) for axis in range(len(extent))]
    result = result.at[tuple(index_at)].set(smallest)
    longest = extent.index(max(extent))
    index_at[longest] = (index_at[longest] + 1) % extent[longest]
    return result.at[tuple(index_at)].set(top_value)


def steps_of(rng, shape, shards, least, high):
    loudness, own = 1.0, jax.random.fold_in(rng, 6)
    for axis_at, blocks in shards:
        draws = jnp.exp(jax.random.uniform(jax.random.fold_in(own, axis_at), (blocks,), jnp.float32, least / len(shards), high / len(shards)))
        loudness = loudness * jnp.repeat(draws, shape[axis_at] // blocks).reshape([-1 if axis == axis_at else 1 for axis in range(len(shape))])
    return loudness


def scatter_about(key, extent, spread, limit, split=(), held_as=jnp.bfloat16):
    array = jax.random.normal(key, extent, jnp.float32) * spread
    if len(split) > 0:
        array = steps_of(key, extent, split, -0.22, 0.18) * array
    return jnp.clip(array, min=-limit, max=limit).astype(held_as)


def setup_inputs(seed: int = 0) -> dict:
    arg_keys = jax.random.split(jax.random.key(seed), 4)
    signal = scatter_about(arg_keys[0], (KZ, 2, NY, SNAP, NXW), 1.0, 6.0, ((2, 8), (4, 4)))
    kx_index = plant(jax.random.randint(arg_keys[1], (K,), 0, NXW // 2), jax.random.fold_in(arg_keys[1], 1), 0, (NXW // 2) - 1).astype(jnp.int32)
    kz_index = plant(jax.random.randint(arg_keys[2], (K,), 0, KZ), jax.random.fold_in(arg_keys[2], 1), 0, KZ - 1).astype(jnp.int32)
    return dict(signal=signal, kx_index=kx_index, kz_index=kz_index)


def tables(kx_values, positions):
    phase = (kx_values[:, None] * positions[None, :]) % NXW
    angle = (2.0 * math.pi / NXW) * phase.astype(jnp.float32)
    factor = float(NXW) ** -0.5
    return (jnp.cos(angle) * factor).astype(jnp.bfloat16), (jnp.sin(angle) * factor).astype(jnp.bfloat16)


def reference(signal, kx_index, kz_index):
    modes, parts, planes, snaps, points = signal.shape
    flat = signal.reshape(modes, parts * planes * snaps, points)
    cosine, sine = tables(kx_index, jnp.arange(points, dtype=jnp.int32))

    def single(item):
        cos_row, sin_row, mode = item
        chosen = lax.dynamic_index_in_dim(flat, mode, 0, keepdims=False)
        basis = jnp.stack([cos_row, sin_row], 1)
        product = jnp.dot(chosen, basis, preferred_element_type=jnp.float32).reshape(2, planes * snaps, 2)
        real = product[0, :, 0] + product[1, :, 1]
        imag = product[1, :, 0] - product[0, :, 1]
        return jnp.stack([real, imag])

    spectra = lax.map(single, (cosine, sine, kz_index)).reshape(-1, 2, planes, snaps)
    first = spectra[:, 0]
    second = spectra[:, 1]
    high = lax.Precision.HIGHEST
    real = (jnp.einsum('kys,kzs->kyz', first, first, precision=high) + jnp.einsum('kys,kzs->kyz', second, second, precision=high)) / SNAP
    imag = (jnp.einsum('kys,kzs->kyz', second, first, precision=high) - jnp.einsum('kys,kzs->kyz', first, second, precision=high)) / SNAP
    return jnp.stack([real, imag])
```

```python
import functools
import math

import jax
import jax.numpy as jnp
from jax import lax
from jax.experimental import pallas as pl
from jax.experimental.pallas import tpu as pltpu
from jax.sharding import PartitionSpec as P

LANES = 128
ROWS = 256
VMEM_BYTES = 66_000_000


def angle_tables(kx_index, kz_index, modes, width, shards, me):
    total = width * shards
    pairs = kx_index.shape[0]
    kk = pairs // shards // 2

    def columns(v):
        v = jnp.broadcast_to(v.reshape(shards, 2, 1, kk), (shards, 2, 2, kk))
        return v.reshape(1, 2 * pairs)

    kx, kz = columns(kx_index), columns(kz_index)
    shift = jnp.broadcast_to(jnp.arange(2, dtype=jnp.int32).reshape(1, 1, 2, 1) * (total // 4), (shards, 2, 2, kk)).reshape(1, 2 * pairs)
    step = 2.0 * math.pi / total
    low = ((kx * jnp.arange(LANES, dtype=jnp.int32)[:, None] + shift) % total).astype(jnp.float32) * step
    at = me * width + LANES * jnp.arange(width // LANES, dtype=jnp.int32)
    high = ((kx * at[:, None]) % total).astype(jnp.float32) * step
    factor = float(total) ** -0.5
    c, s = jnp.cos(low) * factor, jnp.sin(low) * factor
    base = jnp.stack([jnp.stack([c, s]), jnp.stack([-s, c])], 1)
    mask = (kz == jnp.arange(modes, dtype=jnp.int32)[:, None]).astype(jnp.float32)[:, None, None, :]
    turn = jnp.stack([jnp.cos(high), jnp.sin(high)], 1)[None] * mask
    return base, turn


def transform_kernel(chunks, jcs, hs, base, turn, signal, out, xbuf, bbuf, acc, sems):
    def copy(y, q):
        return pltpu.make_async_copy(signal.at[q, pl.ds(y * ROWS, ROWS)], xbuf.at[y, q], sems.at[y, q])

    for y in range(chunks):
        @pl.loop(0, jcs)
        def _(q):
            copy(y, q).start()

    @pl.loop(0, jcs)
    def _(q):
        j, c = q // 2, q % 2

        @pl.loop(0, hs)
        def _(h):
            t = turn[j, h]
            v = base[c, 0] * t[0:1] + base[c, 1] * t[1:2]
            bbuf[q, pl.ds(pl.multiple_of(h * LANES, LANES), LANES)] = v.astype(jnp.bfloat16)

    for y in range(chunks):
        acc[...] = jnp.zeros_like(acc)

        @pl.loop(0, jcs)
        def _(q):
            copy(y, q).wait()
            acc[...] += jnp.dot(xbuf[y, q], bbuf[q], preferred_element_type=jnp.float32)

        out[:, y * ROWS:(y + 1) * ROWS] = acc[...].T


def gram_kernel(per, snaps, own, full, out):
    lane = lax.broadcasted_iota(jnp.int32, (1, LANES), 1)
    first = lane < LANES // 2
    is_re = (lane % (2 * snaps)) < snaps
    for i in range(per):
        mine = own[:, i, :] * (1.0 / snaps)
        right = full[:, i, :].astype(jnp.bfloat16)
        swap = jnp.where(is_re, pltpu.roll(mine, LANES - snaps, 1), -pltpu.roll(mine, snaps, 1))
        zero = jnp.zeros_like(mine)
        left = jnp.concatenate([jnp.where(first, mine, zero), jnp.where(first, zero, mine),
                                jnp.where(first, swap, zero), jnp.where(first, zero, swap)], 0)
        hi = left.astype(jnp.bfloat16)
        lo = (left - hi.astype(jnp.float32)).astype(jnp.bfloat16)
        dims = (((1,), (1,)), ((), ()))
        got = lax.dot_general(jnp.concatenate([hi, lo], 1), jnp.concatenate([right, right], 1), dims,
                              preferred_element_type=jnp.float32)
        out[:, :, i] = got.reshape(2, 2, mine.shape[0], full.shape[0])


def gram(own, full, snaps):
    planes, kk, _ = own.shape
    total = full.shape[0]
    per = kk if kk < 8 else 8
    return pl.pallas_call(
        functools.partial(gram_kernel, per, snaps),
        grid=(kk // per,),
        in_specs=[pl.BlockSpec((planes, per, LANES), lambda g: (0, g, 0)),
                  pl.BlockSpec((total, per, LANES), lambda g: (0, g, 0))],
        out_specs=pl.BlockSpec((2, 2, per, planes, total), lambda g: (0, 0, g, 0, 0)),
        out_shape=jax.ShapeDtypeStruct((2, 2, kk, planes, total), jnp.float32),
    )(own, full)


def on_device(signal, kx_index, kz_index):
    modes, parts, planes, snaps, width = signal.shape
    shards = lax.axis_size("spec")
    me = lax.axis_index("spec")
    pairs = kx_index.shape[0]
    kk = pairs // shards // 2
    jcs, rows, cols, hs = modes * parts, planes * snaps, 2 * pairs, width // LANES
    chunks = rows // ROWS
    base, turn = angle_tables(kx_index, kz_index, modes, width, shards, me)
    partial = pl.pallas_call(
        functools.partial(transform_kernel, chunks, jcs, hs),
        in_specs=[pl.BlockSpec(memory_space=pltpu.VMEM)] * 2 + [pl.BlockSpec(memory_space=pl.ANY)],
        out_specs=pl.BlockSpec(memory_space=pltpu.VMEM),
        out_shape=jax.ShapeDtypeStruct((cols, rows), jnp.float32),
        scratch_shapes=[
            pltpu.VMEM((chunks, jcs, ROWS, width), jnp.bfloat16),
            pltpu.VMEM((jcs, width, cols), jnp.bfloat16),
            pltpu.VMEM((ROWS, cols), jnp.float32),
            pltpu.SemaphoreType.DMA((chunks, jcs)),
        ],
        compiler_params=pltpu.CompilerParams(vmem_limit_bytes=VMEM_BYTES),
    )(base, turn, signal.reshape(jcs, rows, width))
    local = lax.psum_scatter(partial, "spec", scatter_dimension=0, tiled=True)
    own = local.reshape(2, 2, kk, planes, snaps).transpose(3, 2, 0, 1, 4).reshape(planes, kk, 4 * snaps)
    full = lax.all_gather(own, "wall", axis=0, tiled=True)
    out = gram(own, full, snaps)
    return out.reshape(2, 2 * kk, planes, full.shape[0])


def solution(mesh):
    return jax.shard_map(
        on_device,
        mesh=mesh,
        in_specs=(P(None, None, "wall", None, "spec"), P(), P()),
        out_specs=P(None, "spec", "wall", None),
        check_vma=False,
    )
```
